32 devices in a mesh: beam: 8 (over z, x), tm: 4 (over y, core).
Axes of the slice: x: 2, y: 2, z: 4, core: 2. Of those that a mesh axis runs over, the one named last changes fastest.
Arguments:
- voltages: float32 [8, 2, 2, 64, 8192], P('beam', None, None, 'tm'), may hold values from -20 to 20
- filter_taps: float32 [8, 8192], replicated, may hold values from -2 to 2
Outputs:
- cleaned: float32 [8, 2, 64, 8192], P('beam', None, 'tm')
The draws below stay inside these ranges and needn't reach their ends.
All inputs are finite; a program needn't handle non-finite values.
Results may differ from the reference program's by a relative error of at most 0.000058.
Values sent between devices are 32-bit elements; how exact they have to be, the bound alone decides.
A program may use at most 64 MiB of HBM per device.

```python
import math
import jax
import jax.numpy as jnp
from jax import lax

CHANNELS = 8192
TAPS = 8
FRAMES = 64
BEAMS = 8


def draw_voltages(key, part):
    noise_key = jax.random.fold_in(jax.random.fold_in(key, 17), 0)
    shape = (BEAMS, 2, 2, FRAMES, CHANNELS)
    base = jnp.clip(jax.random.normal(noise_key, shape, jnp.float32), -6.0, 6.0) * 0.5
    beam_pos = jnp.arange(BEAMS, dtype=jnp.float32).reshape(BEAMS, 1, 1, 1, 1) / max(BEAMS - 1, 1)
    sample_pos = (jnp.arange(FRAMES, dtype=jnp.float32)[:, None] * CHANNELS + jnp.arange(CHANNELS, dtype=jnp.float32)[None, :]) / (FRAMES * CHANNELS)
    gain = jnp.exp(0.5 * math.log(3.0) * beam_pos + 0.5 * math.log(10.0) * sample_pos[None, None, None])
    return base * gain


def noise(own_key, extent, deviation, limit, held_as=jnp.bfloat16):
    return jnp.clip(deviation * jax.random.normal(own_key, extent, jnp.float32), -limit, limit).astype(held_as)


def setup_inputs(seed: int = 0) -> dict:
    arg_keys = jax.random.split(jax.random.key(seed), 3)
    return {
        "voltages": draw_voltages(jax.random.fold_in(arg_keys[2], 71), 0),
        "filter_taps": noise(arg_keys[1], (TAPS, CHANNELS), TAPS ** -0.5, 2.0, jnp.float32),
    }


def reference(voltages, filter_taps):

    def one_beam(beam_volts):
        padded = jnp.concatenate([beam_volts, jnp.zeros((2, 2, TAPS - 1, CHANNELS), beam_volts.dtype)], axis=2)
        filtered = jnp.zeros_like(beam_volts)
        for tap_index in range(TAPS):
            filtered = filtered + filter_taps[tap_index] * padded[:, :, tap_index:tap_index + FRAMES]
        spectrum = jnp.fft.fft(filtered[:, 0] + 1j * filtered[:, 1], axis=-1) / math.sqrt(CHANNELS)
        return jnp.real(spectrum) ** 2 + jnp.imag(spectrum) ** 2
    powers = lax.map(one_beam, voltages)
    channel_sum = lax.optimization_barrier(jnp.sum(lax.optimization_barrier(jnp.sum(powers, axis=2)) / FRAMES, axis=0))
    return powers - channel_sum[None, :, None, :] / BEAMS
```

```python
import functools
import math

import jax
import jax.numpy as jnp
from jax import lax
from jax.experimental import pallas as pl
from jax.experimental.pallas import tpu as pltpu
from jax.sharding import PartitionSpec as P

RADIX = 128


def passed_along(x, axis, by):
    devices = lax.axis_size(axis)
    pairs = [(i, i + by) for i in range(devices) if 0 <= i + by < devices]
    return lax.ppermute(x, axis, pairs)


def twiddles(rows_count, cols_count, modulus):
    product = (
        jnp.arange(rows_count, dtype=jnp.int32)[:, None]
        * jnp.arange(cols_count, dtype=jnp.int32)[None, :]
        % modulus
    )
    angles = product.astype(jnp.float32) * (-2.0 * math.pi / modulus)
    return (jnp.cos(angles), jnp.sin(angles))


def complex_apply(form, table_cos, table_sin, real_part, imag_part):

    def apply(table, values):
        return jnp.einsum(form, table, values, precision=lax.Precision.HIGH)

    return (
        apply(table_cos, real_part) - apply(table_sin, imag_part),
        apply(table_cos, imag_part) + apply(table_sin, real_part),
    )


def tap_sum(filter_taps, source, count):
    result = filter_taps[0] * source[:, :, 0:count]
    for tap_index in range(1, filter_taps.shape[0]):
        result = result + filter_taps[tap_index] * source[:, :, tap_index : tap_index + count]
    return result


def remote(src, dst, send, recv, beam, tm):
    return pltpu.make_async_remote_copy(
        src_ref=src, dst_ref=dst, send_sem=send, recv_sem=recv,
        device_id=(beam, tm), device_id_type=pl.DeviceIdType.MESH,
    )


def greet(beams, tms):
    b, t = lax.axis_index("beam"), lax.axis_index("tm")
    barrier = pltpu.get_barrier_semaphore()
    for d in range(1, tms):
        pl.semaphore_signal(barrier, inc=1, device_id=(b, lax.rem(t + d, tms)), device_id_type=pl.DeviceIdType.MESH)
    for d in range(1, beams):
        pl.semaphore_signal(barrier, inc=1, device_id=(lax.rem(b + d, beams), t), device_id_type=pl.DeviceIdType.MESH)
    pl.semaphore_wait(barrier, tms - 1 + beams - 1)


def total_all(beams, tms, tot, res, part, whole, in_tm, in_beam, sems):
    b, t = lax.axis_index("beam"), lax.axis_index("tm")
    rows = tot.shape[0] // tms
    s1, r1, s2, r2, s3, r3 = sems

    def block(i):
        return pl.ds(pl.multiple_of(i * rows, rows), rows)

    copies = []
    for d in range(1, tms):
        peer = lax.rem(t + d, tms)
        copies.append(remote(tot.at[block(peer)], in_tm.at[d - 1], s1.at[d - 1], r1.at[d - 1], b, peer))
        copies[-1].start()
    own = tot[block(t), :]
    for d in range(1, tms):
        copies[d - 1].wait_recv()
        own = own + in_tm[d - 1]
    part[...] = own
    second = []
    for d in range(1, beams):
        peer = lax.rem(b + d, beams)
        second.append(remote(part, in_beam.at[d - 1], s2.at[d - 1], r2.at[d - 1], peer, t))
        second[-1].start()
    for d in range(1, beams):
        second[d - 1].wait_recv()
        own = own + in_beam[d - 1]
    whole[...] = own
    third = []
    for d in range(1, tms):
        peer = lax.rem(t + d, tms)
        third.append(remote(whole, res.at[block(t)], s3.at[d - 1], r3.at[d - 1], b, peer))
        third[-1].start()
    res[block(t), :] = own
    for c in third:
        c.wait_recv()
    for c in copies + second + third:
        c.wait_send()


def total_scratch(beams, tms, rows):
    share = (rows // tms, 128)
    sem = pltpu.SemaphoreType.DMA
    return [
        pltpu.VMEM(share, jnp.float32),
        pltpu.VMEM(share, jnp.float32),
        pltpu.VMEM((tms - 1, *share), jnp.float32),
        pltpu.VMEM((beams - 1, *share), jnp.float32),
        sem((tms - 1,)), sem((tms - 1,)), sem((beams - 1,)), sem((beams - 1,)), sem((tms - 1,)), sem((tms - 1,)),
    ]


def total_kernel(beams, tms, tot, res, part, whole, in_tm, in_beam, *sems):
    greet(beams, tms)
    total_all(beams, tms, tot, res, part, whole, in_tm, in_beam, sems)


def total_of_all(tot):
    beams, tms = lax.axis_size("beam"), lax.axis_size("tm")
    return pl.pallas_call(
        functools.partial(total_kernel, beams, tms),
        out_shape=jax.ShapeDtypeStruct(tot.shape, tot.dtype),
        in_specs=[pl.BlockSpec(memory_space=pltpu.VMEM)],
        out_specs=pl.BlockSpec(memory_space=pltpu.VMEM),
        scratch_shapes=total_scratch(beams, tms, tot.shape[0]),
        compiler_params=pltpu.CompilerParams(collective_id=0, has_side_effects=True),
        name="total_of_all",
    )(tot)


def body(voltages, filter_taps):
    segment = voltages[0]
    frames = segment.shape[2]
    channels = segment.shape[3]
    rim_frames = filter_taps.shape[0] - 1
    zero_rim = jnp.zeros((2, 2, rim_frames, channels), jnp.float32)
    padded = jnp.concatenate([segment, zero_rim], axis=2)
    filtered = tap_sum(filter_taps, padded, frames)
    leading_rows = jnp.concatenate([zero_rim, segment[:, :, :rim_frames]], axis=2)
    partial_value = tap_sum(filter_taps, leading_rows, rim_frames)
    incoming = passed_along(partial_value, "tm", -1)
    filtered = filtered.at[:, :, frames - rim_frames :].add(incoming)
    stride = channels // RADIX
    grid_real = filtered[:, 0].reshape(2, frames, RADIX, stride)
    grid_imag = filtered[:, 1].reshape(2, frames, RADIX, stride)
    cos_first, sin_first = twiddles(RADIX, RADIX, RADIX)
    section_real, section_imag = complex_apply(
        "kn,pfnm->pfmk", cos_first, sin_first, grid_real, grid_imag
    )
    twist_cos, twist_sin = twiddles(stride, RADIX, channels)
    twisted_real = section_real * twist_cos - section_imag * twist_sin
    twisted_imag = section_real * twist_sin + section_imag * twist_cos
    cos_second, sin_second = twiddles(stride, stride, stride)
    spec_real, spec_imag = complex_apply(
        "jm,pfmk->pfjk", cos_second, sin_second, twisted_real, twisted_imag
    )
    powers = ((spec_real * spec_real + spec_imag * spec_imag) / channels).reshape(
        2, frames, channels
    )
    totals = jnp.sum(powers, axis=1)
    channel_sum = total_of_all(totals.reshape(-1, 128)).reshape(totals.shape)
    all_frames = frames * lax.axis_size("tm")
    all_beams = voltages.shape[0] * lax.axis_size("beam")
    baseline = channel_sum / all_frames / all_beams
    return (powers - baseline[:, None, :])[None]


def solution(mesh):
    placed = (P("beam", None, None, "tm", None), P())
    return jax.shard_map(
        body, mesh=mesh, in_specs=placed, out_specs=P("beam", None, "tm", None), check_vma=False
    )
```

```python
import functools
import math

import jax
import jax.numpy as jnp
import numpy as np
from jax import lax
from jax.experimental import pallas as pl
from jax.experimental.pallas import tpu as pltpu
from jax.sharding import PartitionSpec as P

LANES = 128
GROUP = 8


def passed_along(x, axis, by):
    devices = lax.axis_size(axis)
    pairs = [(i, i + by) for i in range(devices) if 0 <= i + by < devices]
    return lax.ppermute(x, axis, pairs)


def remote(src, dst, send, recv, beam, tm):
    return pltpu.make_async_remote_copy(
        src_ref=src, dst_ref=dst, send_sem=send, recv_sem=recv,
        device_id=(beam, tm), device_id_type=pl.DeviceIdType.MESH,
    )


def greet(beams, tms):
    b, t = lax.axis_index("beam"), lax.axis_index("tm")
    barrier = pltpu.get_barrier_semaphore()
    for d in range(1, tms):
        pl.semaphore_signal(barrier, inc=1, device_id=(b, lax.rem(t + d, tms)), device_id_type=pl.DeviceIdType.MESH)
    for d in range(1, beams):
        pl.semaphore_signal(barrier, inc=1, device_id=(lax.rem(b + d, beams), t), device_id_type=pl.DeviceIdType.MESH)
    pl.semaphore_wait(barrier, tms - 1 + beams - 1)


def total_all(beams, tms, tot, res, part, whole, in_tm, in_beam, sems):
    b, t = lax.axis_index("beam"), lax.axis_index("tm")
    rows = tot.shape[0] // tms
    s1, r1, s2, r2, s3, r3 = sems

    def block(i):
        return pl.ds(pl.multiple_of(i * rows, rows), rows)

    copies = []
    for d in range(1, tms):
        peer = lax.rem(t + d, tms)
        copies.append(remote(tot.at[block(peer)], in_tm.at[d - 1], s1.at[d - 1], r1.at[d - 1], b, peer))
        copies[-1].start()
    own = tot[block(t), :]
    for d in range(1, tms):
        copies[d - 1].wait_recv()
        own = own + in_tm[d - 1]
    part[...] = own
    second = []
    for d in range(1, beams):
        peer = lax.rem(b + d, beams)
        second.append(remote(part, in_beam.at[d - 1], s2.at[d - 1], r2.at[d - 1], peer, t))
        second[-1].start()
    for d in range(1, beams):
        second[d - 1].wait_recv()
        own = own + in_beam[d - 1]
    whole[...] = own
    third = []
    for d in range(1, tms):
        peer = lax.rem(t + d, tms)
        third.append(remote(whole, res.at[block(t)], s3.at[d - 1], r3.at[d - 1], b, peer))
        third[-1].start()
    res[block(t), :] = own
    for c in third:
        c.wait_recv()
    for c in copies + second + third:
        c.wait_send()


def total_scratch(beams, tms, rows):
    share = (rows // tms, 128)
    sem = pltpu.SemaphoreType.DMA
    return [
        pltpu.VMEM(share, jnp.float32),
        pltpu.VMEM(share, jnp.float32),
        pltpu.VMEM((tms - 1, *share), jnp.float32),
        pltpu.VMEM((beams - 1, *share), jnp.float32),
        sem((tms - 1,)), sem((tms - 1,)), sem((beams - 1,)), sem((beams - 1,)), sem((tms - 1,)), sem((tms - 1,)),
    ]


def total_kernel(beams, tms, tot, res, part, whole, in_tm, in_beam, *sems):
    greet(beams, tms)
    total_all(beams, tms, tot, res, part, whole, in_tm, in_beam, sems)


def total_of_all(tot):
    beams, tms = lax.axis_size("beam"), lax.axis_size("tm")
    return pl.pallas_call(
        functools.partial(total_kernel, beams, tms),
        out_shape=jax.ShapeDtypeStruct(tot.shape, tot.dtype),
        in_specs=[pl.BlockSpec(memory_space=pltpu.VMEM)],
        out_specs=pl.BlockSpec(memory_space=pltpu.VMEM),
        scratch_shapes=total_scratch(beams, tms, tot.shape[0]),
        compiler_params=pltpu.CompilerParams(collective_id=0, has_side_effects=True),
        name="total_of_all",
    )(tot)


def tables(channels):
    tiles = channels // LANES
    angle = 2.0 * math.pi * (np.outer(np.arange(tiles), np.arange(LANES)) % channels) / channels
    scale = channels ** -0.5
    k2 = np.concatenate([np.arange(0, LANES, 2), np.arange(1, LANES, 2)])
    last = 2.0 * math.pi * (np.outer(np.arange(LANES), k2) % LANES) / LANES
    c, s = np.cos(last), np.sin(last)
    matrix = jnp.asarray(np.block([[c, -s], [s, c]]).astype(np.float32))
    high = matrix.astype(jnp.bfloat16)
    low = (matrix - high.astype(jnp.float32)).astype(jnp.bfloat16)
    return (
        jnp.asarray((scale * np.cos(angle)).astype(np.float32)),
        jnp.asarray((-scale * np.sin(angle)).astype(np.float32)),
        high,
        low,
    )


def times(x, turn, of):
    turn = turn % of
    re, im = x
    if turn == 0:
        return x
    if 4 * turn == of:
        return im, -re
    if 2 * turn == of:
        return -re, -im
    if 4 * turn == 3 * of:
        return -im, re
    c, s = math.cos(2 * math.pi * turn / of), math.sin(2 * math.pi * turn / of)
    if 8 * turn % of == 0:
        h = abs(c)
        if 8 * turn == of:
            return (re + im) * h, (im - re) * h
        if 8 * turn == 3 * of:
            return (im - re) * h, (re + im) * -h
    return re * c + im * s, im * c - re * s


def add(x, y):
    return x[0] + y[0], x[1] + y[1]


def sub(x, y):
    return x[0] - y[0], x[1] - y[1]


def transform(xs):
    n = len(xs)
    if n == 1:
        return xs
    even, odd = transform(xs[0::2]), transform(xs[1::2])
    odd = [times(o, k, n) for k, o in enumerate(odd)]
    return [add(e, o) for e, o in zip(even, odd)] + [sub(e, o) for e, o in zip(even, odd)]


def channelize(lo, hi, taps, tw_re, tw_im, high, low, xs, mid, rows_h, rows_l, pw, turned):
    tap_count, channels = taps.shape
    tiles = channels // LANES
    outer = 8
    inner = tiles // outer

    def first(b, carry):
        tiles_out = []
        for a in range(outer):
            cols = pl.ds(pl.multiple_of((a * inner + b) * LANES, LANES), LANES)
            weights = taps[:, cols]
            pair = []
            for q in range(2):
                base = (a * 2 + q) * 2 * GROUP
                xs[base : base + GROUP, :] = lo[q, :, cols]
                xs[base + GROUP : base + 2 * GROUP, :] = hi[q, :, cols]
                total = weights[0:1] * lo[q, :, cols]
                for t in range(1, tap_count):
                    total = total + weights[t : t + 1] * xs[base + t : base + t + GROUP, :]
                pair.append(total)
            tiles_out.append(tuple(pair))
        for c, z in enumerate(transform(tiles_out)):
            at = pl.ds(pl.multiple_of((c * inner + b) * GROUP, GROUP), GROUP)
            mid[0, at, :] = z[0]
            mid[1, at, :] = z[1]
        return carry

    lax.fori_loop(0, inner, first, 0)

    for c0 in range(0, outer, 2):
        both = []
        for c in (c0, c0 + 1):
            zs = []
            for b in range(inner):
                at = slice((c * inner + b) * GROUP, (c * inner + b + 1) * GROUP)
                zs.append(times((mid[0, at, :], mid[1, at, :]), b * c, tiles))
            turned_out = []
            for d, (re, im) in enumerate(transform(zs)):
                k1 = c + outer * d
                wr, wi = tw_re[k1 : k1 + 1, :], tw_im[k1 : k1 + 1, :]
                turned_out.append((re * wr - im * wi, re * wi + im * wr))
            both.append(turned_out)
        for d in range(inner):
            at = slice((c0 + outer * d) * GROUP, (c0 + outer * d + 2) * GROUP)
            for q in range(2):
                x = jnp.concatenate([both[0][d][q], both[1][d][q]], axis=0)
                h = x.astype(jnp.bfloat16)
                rows_h[at, q * LANES : (q + 1) * LANES] = h
                rows_l[at, q * LANES : (q + 1) * LANES] = (x - h.astype(jnp.float32)).astype(jnp.bfloat16)

    def dot(x, y):
        return jnp.dot(x, y, preferred_element_type=jnp.float32)

    spec = dot(rows_h[...], high[...]) + dot(rows_l[...], high[...]) + dot(rows_h[...], low[...])
    spec_re, spec_im = spec[:, :LANES], spec[:, LANES:]
    pw[...] = spec_re * spec_re + spec_im * spec_im

    left = lax.broadcasted_iota(jnp.int32, (tiles, LANES), 1) < tiles
    total = jnp.zeros((tiles, LANES), jnp.float32)
    for f in range(0, GROUP, 2):
        pair = jnp.concatenate(
            [pw[pl.ds(f, tiles, stride=GROUP), :], pw[pl.ds(f + 1, tiles, stride=GROUP), :]], axis=0
        ).T
        upper, lower = pair[:tiles], pair[tiles:]
        one = jnp.where(left, upper, pltpu.roll(lower, tiles, 1))
        two = jnp.where(left, pltpu.roll(upper, tiles, 1), lower)
        total = total + one + two
        turned[pl.ds(f, tiles, stride=GROUP), :] = one
        turned[pl.ds(f + 1, tiles, stride=GROUP), :] = two
    return total


def power_kernel(lo, hi, taps, tw_re, tw_im, high, low, so_far, *rest):
    powers, total, *scratch = rest[-8:]
    turned = scratch[-1]
    part = channelize(lo.at[0], hi.at[0], taps, tw_re, tw_im, high, low, *scratch)
    first = pl.program_id(1) == 0

    @pl.when(first)
    def _():
        total[0] = so_far[0] + part

    @pl.when(jnp.logical_not(first))
    def _():
        total[0] = total[0] + part

    for j in range(part.shape[0]):
        powers[0, :, j * LANES : (j + 1) * LANES] = turned[j * GROUP : (j + 1) * GROUP, :]


def powers_of(lo, lo_at, hi, hi_at, taps, consts, so_far, powers, grid, out_at):
    channels = taps.shape[1]
    tiles = channels // LANES
    rows = tiles * GROUP
    block = (1, 2, GROUP, channels)
    whole = pl.BlockSpec(memory_space=pltpu.VMEM)
    total_spec = pl.BlockSpec((1, tiles, LANES), lambda p, g: (out_at(p, g)[0], 0, 0))
    earlier = [] if powers is None else [powers]
    return pl.pallas_call(
        power_kernel,
        grid=grid,
        out_shape=(
            jax.ShapeDtypeStruct((lo.shape[0], lo.shape[2], channels), jnp.float32),
            jax.ShapeDtypeStruct(so_far.shape, so_far.dtype),
        ),
        in_specs=[
            pl.BlockSpec(block, lo_at),
            pl.BlockSpec(block, hi_at),
            whole, whole, whole, whole, whole,
            total_spec,
        ]
        + [pl.BlockSpec(memory_space=pl.ANY) for _ in earlier],
        out_specs=(
            pl.BlockSpec((1, GROUP, channels), lambda p, g: (*out_at(p, g), 0)),
            total_spec,
        ),
        scratch_shapes=[
            pltpu.VMEM((8 * 2 * 2 * GROUP, LANES), jnp.float32),
            pltpu.VMEM((2, rows, LANES), jnp.float32),
            pltpu.VMEM((rows, 2 * LANES), jnp.bfloat16),
            pltpu.VMEM((rows, 2 * LANES), jnp.bfloat16),
            pltpu.VMEM((rows, LANES), jnp.float32),
            pltpu.VMEM((rows, LANES), jnp.float32),
        ],
        input_output_aliases={7: 1, 8: 0} if earlier else {7: 1},
        cost_estimate=pl.CostEstimate(
            flops=grid[0] * grid[1] * 1200 * 1000 * 1000,
            bytes_accessed=grid[0] * grid[1] * 5 * GROUP * channels * 4,
            transcendentals=0,
        ),
        name="powers_of",
    )(lo, hi, taps, *consts, so_far, *earlier)


def remove_kernel(scale, powers, sums, out):
    for j in range(sums.shape[0]):
        at = slice(j * LANES, (j + 1) * LANES)
        out[0, 0, :, at] = powers[0, :, at] - sums[j : j + 1, :] * scale


def removed(powers, sums, scale):
    pols, frames, channels = powers.shape
    tiles = channels // LANES
    return pl.pallas_call(
        functools.partial(remove_kernel, scale),
        grid=(pols, frames // GROUP),
        out_shape=jax.ShapeDtypeStruct((1, *powers.shape), powers.dtype),
        in_specs=[
            pl.BlockSpec((1, GROUP, channels), lambda p, g: (p, g, 0)),
            pl.BlockSpec((tiles, LANES), lambda p, g: (p, 0)),
        ],
        out_specs=pl.BlockSpec((1, 1, GROUP, channels), lambda p, g: (0, p, g, 0)),
        name="removed",
    )(powers, sums)


def body(voltages, filter_taps):
    segment = voltages[0]
    pols, _, frames, channels = segment.shape
    groups = frames // GROUP
    tiles = channels // LANES
    consts = tables(channels)
    rims = [passed_along(segment[p : p + 1, :, :GROUP], "tm", -1) for p in range(pols)]
    total = jnp.zeros((pols, tiles, LANES), jnp.float32)
    powers, total = powers_of(
        segment, lambda p, g: (p, 0, g, 0), segment, lambda p, g: (p, 0, g + 1, 0),
        filter_taps, consts, total, None, (pols, groups - 1), lambda p, g: (p, g),
    )
    for p in range(pols):
        powers, total = powers_of(
            segment, lambda _, g, p=p: (p, 0, groups - 1, 0), rims[p], lambda _, g: (0, 0, 0, 0),
            filter_taps, consts, total, powers, (1, 1), lambda _, g, p=p: (p, groups - 1),
        )
    sums = total_of_all(total.reshape(pols * tiles, LANES))
    all_frames = frames * lax.axis_size("tm")
    all_beams = voltages.shape[0] * lax.axis_size("beam")
    return removed(powers, sums, 1.0 / (all_frames * all_beams))


def solution(mesh):
    placed = (P("beam", None, None, "tm", None), P())
    return jax.shard_map(
        body, mesh=mesh, in_specs=placed, out_specs=P("beam", None, "tm", None), check_vma=False
    )
```

```python
import functools
import math

import jax
import jax.numpy as jnp
import numpy as np
from jax import lax
from jax.experimental import pallas as pl
from jax.experimental.pallas import tpu as pltpu
from jax.sharding import PartitionSpec as P

LANES = 128
GROUP = 8


def remote(src, dst, send, recv, beam, tm):
    return pltpu.make_async_remote_copy(
        src_ref=src, dst_ref=dst, send_sem=send, recv_sem=recv,
        device_id=(beam, tm), device_id_type=pl.DeviceIdType.MESH,
    )


def greet(beams, tms):
    b, t = lax.axis_index("beam"), lax.axis_index("tm")
    barrier = pltpu.get_barrier_semaphore()
    for d in range(1, tms):
        pl.semaphore_signal(barrier, inc=1, device_id=(b, lax.rem(t + d, tms)), device_id_type=pl.DeviceIdType.MESH)
    for d in range(1, beams):
        pl.semaphore_signal(barrier, inc=1, device_id=(lax.rem(b + d, beams), t), device_id_type=pl.DeviceIdType.MESH)
    pl.semaphore_wait(barrier, tms - 1 + beams - 1)


class Total:
    def __init__(self, beams, tms, tot, res, first_row, count, part, whole, in_tm, in_beam, sems):
        self.beams, self.tms, self.tot, self.res = beams, tms, tot, res
        self.first_row, self.rows = first_row, count // tms
        self.part, self.whole, self.in_tm, self.in_beam, self.sems = part, whole, in_tm, in_beam, sems
        self.b, self.t = lax.axis_index("beam"), lax.axis_index("tm")
        self.sent = []

    def block(self, i):
        return pl.ds(pl.multiple_of(self.first_row + i * self.rows, self.rows), self.rows)

    def to_tm(self):
        s1, r1 = self.sems[:2]
        self.first = []
        for d in range(1, self.tms):
            peer = lax.rem(self.t + d, self.tms)
            self.first.append(remote(
                self.tot.at[self.block(peer)], self.in_tm.at[d - 1], s1.at[d - 1], r1.at[d - 1], self.b, peer))
            self.first[-1].start()

    def to_beams(self):
        s2, r2 = self.sems[2:4]
        own = self.tot[self.block(self.t), :]
        for d, copy in enumerate(self.first):
            copy.wait_recv()
            own = own + self.in_tm[d]
        self.part[...] = own
        self.second = []
        for d in range(1, self.beams):
            peer = lax.rem(self.b + d, self.beams)
            self.second.append(remote(
                self.part, self.in_beam.at[d - 1], s2.at[d - 1], r2.at[d - 1], peer, self.t))
            self.second[-1].start()

    def back(self):
        s3, r3 = self.sems[4:]
        own = self.part[...]
        for d, copy in enumerate(self.second):
            copy.wait_recv()
            own = own + self.in_beam[d]
        self.whole[...] = own
        self.third = []
        for d in range(1, self.tms):
            peer = lax.rem(self.t + d, self.tms)
            self.third.append(remote(
                self.whole, self.res.at[self.block(self.t)], s3.at[d - 1], r3.at[d - 1], self.b, peer))
            self.third[-1].start()
        self.res[self.block(self.t), :] = own

    def arrive(self):
        for copy in self.third:
            copy.wait_recv()

    def leave(self):
        for copy in self.first + self.second + self.third:
            copy.wait_send()


def total_scratch(beams, tms, rows):
    share = (rows // tms, LANES)
    sem = pltpu.SemaphoreType.DMA
    return [
        pltpu.VMEM(share, jnp.float32),
        pltpu.VMEM(share, jnp.float32),
        pltpu.VMEM((tms - 1, *share), jnp.float32),
        pltpu.VMEM((beams - 1, *share), jnp.float32),
        sem((tms - 1,)), sem((tms - 1,)), sem((beams - 1,)), sem((beams - 1,)), sem((tms - 1,)), sem((tms - 1,)),
    ]


TOTAL_SCRATCH = 10


def tables(channels):
    tiles = channels // LANES
    angle = 2.0 * math.pi * (np.outer(np.arange(tiles), np.arange(LANES)) % channels) / channels
    scale = channels ** -0.5
    k2 = np.concatenate([np.arange(0, LANES, 2), np.arange(1, LANES, 2)])
    last = 2.0 * math.pi * (np.outer(np.arange(LANES), k2) % LANES) / LANES
    c, s = np.cos(last), np.sin(last)
    matrix = jnp.asarray(np.block([[c, -s], [s, c]]).astype(np.float32))
    high = matrix.astype(jnp.bfloat16)
    low = (matrix - high.astype(jnp.float32)).astype(jnp.bfloat16)
    return (
        jnp.asarray((scale * np.cos(angle)).astype(np.float32)),
        jnp.asarray((-scale * np.sin(angle)).astype(np.float32)),
        high,
        low,
    )


def times(x, turn, of):
    turn = turn % of
    re, im = x
    if turn == 0:
        return x
    if 4 * turn == of:
        return im, -re
    if 2 * turn == of:
        return -re, -im
    if 4 * turn == 3 * of:
        return -im, re
    c, s = math.cos(2 * math.pi * turn / of), math.sin(2 * math.pi * turn / of)
    if 8 * turn % of == 0:
        h = abs(c)
        if 8 * turn == of:
            return (re + im) * h, (im - re) * h
        if 8 * turn == 3 * of:
            return (im - re) * h, (re + im) * -h
    return re * c + im * s, im * c - re * s


def add(x, y):
    return x[0] + y[0], x[1] + y[1]


def sub(x, y):
    return x[0] - y[0], x[1] - y[1]


def transform(xs):
    n = len(xs)
    if n == 1:
        return xs
    even, odd = transform(xs[0::2]), transform(xs[1::2])
    odd = [times(o, k, n) for k, o in enumerate(odd)]
    return [add(e, o) for e, o in zip(even, odd)] + [sub(e, o) for e, o in zip(even, odd)]


def channelize(lo, hi, taps, tw_re, tw_im, high, low, xs, mid, rows_h, rows_l, pw, turned):
    tap_count, channels = taps.shape
    tiles = channels // LANES
    outer = 8
    inner = tiles // outer

    def first(b, carry):
        tiles_out = []
        for a in range(outer):
            cols = pl.ds(pl.multiple_of((a * inner + b) * LANES, LANES), LANES)
            weights = taps[:, cols]
            pair = []
            for q in range(2):
                base = (a * 2 + q) * 2 * GROUP
                xs[base : base + GROUP, :] = lo[q, :, cols]
                xs[base + GROUP : base + 2 * GROUP, :] = hi[q, :, cols]
                total = weights[0:1] * lo[q, :, cols]
                for t in range(1, tap_count):
                    total = total + weights[t : t + 1] * xs[base + t : base + t + GROUP, :]
                pair.append(total)
            tiles_out.append(tuple(pair))
        for c, z in enumerate(transform(tiles_out)):
            at = pl.ds(pl.multiple_of((c * inner + b) * GROUP, GROUP), GROUP)
            mid[0, at, :] = z[0]
            mid[1, at, :] = z[1]
        return carry

    lax.fori_loop(0, inner, first, 0)

    for c0 in range(0, outer, 2):
        both = []
        for c in (c0, c0 + 1):
            zs = []
            for b in range(inner):
                at = slice((c * inner + b) * GROUP, (c * inner + b + 1) * GROUP)
                zs.append(times((mid[0, at, :], mid[1, at, :]), b * c, tiles))
            turned_out = []
            for d, (re, im) in enumerate(transform(zs)):
                k1 = c + outer * d
                wr, wi = tw_re[k1 : k1 + 1, :], tw_im[k1 : k1 + 1, :]
                turned_out.append((re * wr - im * wi, re * wi + im * wr))
            both.append(turned_out)
        for d in range(inner):
            at = slice((c0 + outer * d) * GROUP, (c0 + outer * d + 2) * GROUP)
            for q in range(2):
                x = jnp.concatenate([both[0][d][q], both[1][d][q]], axis=0)
                h = x.astype(jnp.bfloat16)
                rows_h[at, q * LANES : (q + 1) * LANES] = h
                rows_l[at, q * LANES : (q + 1) * LANES] = (x - h.astype(jnp.float32)).astype(jnp.bfloat16)

    def dot(x, y):
        return jnp.dot(x, y, preferred_element_type=jnp.float32)

    spec = dot(rows_h[...], high[...]) + dot(rows_l[...], high[...]) + dot(rows_h[...], low[...])
    spec_re, spec_im = spec[:, :LANES], spec[:, LANES:]
    pw[...] = spec_re * spec_re + spec_im * spec_im

    left = lax.broadcasted_iota(jnp.int32, (tiles, LANES), 1) < tiles
    total = jnp.zeros((tiles, LANES), jnp.float32)
    for f in range(0, GROUP, 2):
        pair = jnp.concatenate(
            [pw[pl.ds(f, tiles, stride=GROUP), :], pw[pl.ds(f + 1, tiles, stride=GROUP), :]], axis=0
        ).T
        upper, lower = pair[:tiles], pair[tiles:]
        one = jnp.where(left, upper, pltpu.roll(lower, tiles, 1))
        two = jnp.where(left, pltpu.roll(upper, tiles, 1), lower)
        total = total + one + two
        turned[pl.ds(f, tiles, stride=GROUP), :] = one
        turned[pl.ds(f + 1, tiles, stride=GROUP), :] = two
    return total


def kernel(beams, tms, scale, x, *refs):
    from_consts, (powers, base) = refs[:5], refs[5:7]
    refs = refs[7:]
    consts, refs = refs[:5], refs[5:]
    xv, rim, pv, tot, res, load_sem, const_sem, rim_send, rim_recv, out_sem = refs[:10]
    work, refs = refs[10:16], refs[16:]
    pols, _, frames, channels = xv.shape
    groups = frames // GROUP
    tiles = channels // LANES
    turned = work[-1]
    b, t = lax.axis_index("beam"), lax.axis_index("tm")

    loads = [pltpu.make_async_copy(x.at[p], xv.at[p], load_sem.at[p]) for p in range(pols)]
    fetches = [pltpu.make_async_copy(f, c, const_sem.at[i]) for i, (f, c) in enumerate(zip(from_consts, consts))]
    fetches[0].start()
    for copy in loads + fetches[1:]:
        copy.start()
    greet(beams, tms)
    rims = [
        remote(x.at[p, :, 0:GROUP, :], rim.at[p], rim_send.at[p], rim_recv.at[p], b, lax.rem(t + tms - 1, tms))
        for p in range(pols)
    ]

    @pl.when(t > 0)
    def _():
        for copy in rims:
            copy.start()

    @pl.when(t == tms - 1)
    def _():
        rim[...] = jnp.zeros_like(rim)

    for copy in fetches + loads:
        copy.wait()

    def one(p, g, lo, hi):
        part = channelize(lo, hi, *consts, *work)
        at = pl.ds(pl.multiple_of(p * tiles, tiles), tiles)
        if isinstance(p, int):
            tot[at, :] = tot[at, :] + part
        else:
            tot[at, :] = jnp.where(g == 0, part, tot[at, :] + part) if groups > 2 else part
        frames_at = pl.ds(pl.multiple_of(g * GROUP, GROUP), GROUP)
        for j in range(tiles):
            pv[p, frames_at, j * LANES : (j + 1) * LANES] = turned[j * GROUP : (j + 1) * GROUP, :]

    def early(i, carry):
        p, g = i // (groups - 1), lax.rem(i, groups - 1)
        after = pl.multiple_of((g + 1) * GROUP, GROUP)
        one(
            p, g,
            xv.at[p, :, pl.ds(pl.multiple_of(g * GROUP, GROUP), GROUP), :],
            xv.at[p, :, pl.ds(after, GROUP), :],
        )
        return carry

    lax.fori_loop(0, pols * (groups - 1), early, 0)

    outs = []
    totals = []
    for p in range(pols):

        @pl.when(t < tms - 1)
        def _():
            rims[p].wait_recv()

        one(p, groups - 1, xv.at[p, :, frames - GROUP : frames, :], rim.at[p])
        now = refs[p * TOTAL_SCRATCH : (p + 1) * TOTAL_SCRATCH]
        totals.append(Total(beams, tms, tot, res, p * tiles, tiles, *now[:4], now[4:]))
        totals[p].to_tm()
        outs.append(pltpu.make_async_copy(pv.at[p], powers.at[p], out_sem.at[p]))
        outs[p].start()
        if p > 0:
            totals[p - 1].back()
        totals[p].to_beams()
    for p in range(pols):
        if p == pols - 1:
            totals[p].back()
        totals[p].arrive()
        for j in range(tiles):
            row = p * tiles + j
            base[p : p + 1, j * LANES : (j + 1) * LANES] = res[row : row + 1, :] * scale
    for total in totals:
        total.leave()

    @pl.when(t > 0)
    def _():
        for copy in rims:
            copy.wait_send()

    for copy in outs:
        copy.wait()


def powers_and_base(x, taps, scale):
    beams, tms = lax.axis_size("beam"), lax.axis_size("tm")
    pols, _, frames, channels = x.shape
    tiles = channels // LANES
    rows = tiles * GROUP
    consts = (taps, *tables(channels))
    sem = pltpu.SemaphoreType.DMA
    f32 = jnp.float32
    anywhere = pl.BlockSpec(memory_space=pl.ANY)
    return pl.pallas_call(
        functools.partial(kernel, beams, tms, scale),
        out_shape=(
            jax.ShapeDtypeStruct((pols, frames, channels), f32),
            jax.ShapeDtypeStruct((pols, channels), f32),
        ),
        in_specs=[anywhere] * (1 + len(consts)),
        out_specs=(anywhere, pl.BlockSpec(memory_space=pltpu.VMEM)),
        scratch_shapes=[pltpu.VMEM(c.shape, c.dtype) for c in consts]
        + [
            pltpu.VMEM(x.shape, f32),
            pltpu.VMEM((pols, 2, GROUP, channels), f32),
            pltpu.VMEM((pols, frames, channels), f32),
            pltpu.VMEM((pols * tiles, LANES), f32),
            pltpu.VMEM((pols * tiles, LANES), f32),
            sem((pols,)), sem((len(consts),)), sem((pols,)), sem((pols,)), sem((pols,)),
            pltpu.VMEM((8 * 2 * 2 * GROUP, LANES), f32),
            pltpu.VMEM((2, rows, LANES), f32),
            pltpu.VMEM((rows, 2 * LANES), jnp.bfloat16),
            pltpu.VMEM((rows, 2 * LANES), jnp.bfloat16),
            pltpu.VMEM((rows, LANES), f32),
            pltpu.VMEM((rows, LANES), f32),
        ]
        + total_scratch(beams, tms, tiles) * pols,
        compiler_params=pltpu.CompilerParams(collective_id=0, has_side_effects=True),
        name="powers_and_base",
    )(x, *consts)


def body(voltages, filter_taps):
    frames = voltages.shape[3] * lax.axis_size("tm")
    beams = voltages.shape[0] * lax.axis_size("beam")
    powers, base = powers_and_base(voltages[0], filter_taps, 1.0 / (frames * beams))
    return (powers - base[:, None, :])[None]


def solution(mesh):
    placed = (P("beam", None, None, "tm", None), P())
    return jax.shard_map(
        body, mesh=mesh, in_specs=placed, out_specs=P("beam", None, "tm", None), check_vma=False
    )
```

```python
import functools
import math

import jax
import jax.numpy as jnp
import numpy as np
from jax import lax
from jax.experimental import pallas as pl
from jax.experimental.pallas import tpu as pltpu
from jax.sharding import PartitionSpec as P

LANES = 128
GROUP = 8


def remote(src, dst, send, recv, beam, tm):
    return pltpu.make_async_remote_copy(
        src_ref=src, dst_ref=dst, send_sem=send, recv_sem=recv,
        device_id=(beam, tm), device_id_type=pl.DeviceIdType.MESH,
    )


def greet(beams, tms):
    b, t = lax.axis_index("beam"), lax.axis_index("tm")
    barrier = pltpu.get_barrier_semaphore()
    for d in range(1, tms):
        pl.semaphore_signal(barrier, inc=1, device_id=(b, lax.rem(t + d, tms)), device_id_type=pl.DeviceIdType.MESH)
    for d in range(1, beams):
        pl.semaphore_signal(barrier, inc=1, device_id=(lax.rem(b + d, beams), t), device_id_type=pl.DeviceIdType.MESH)
    pl.semaphore_wait(barrier, tms - 1 + beams - 1)


class Total:
    def __init__(self, beams, tms, tot, res, first_row, count, part, whole, in_tm, in_beam, sems):
        self.beams, self.tms, self.tot, self.res = beams, tms, tot, res
        self.first_row, self.rows = first_row, count // tms
        self.part, self.whole, self.in_tm, self.in_beam, self.sems = part, whole, in_tm, in_beam, sems
        self.b, self.t = lax.axis_index("beam"), lax.axis_index("tm")
        self.sent = []

    def block(self, i):
        return pl.ds(pl.multiple_of(self.first_row + i * self.rows, self.rows), self.rows)

    def to_tm(self):
        s1, r1 = self.sems[:2]
        self.first = []
        for d in range(1, self.tms):
            peer = lax.rem(self.t + d, self.tms)
            self.first.append(remote(
                self.tot.at[self.block(peer)], self.in_tm.at[d - 1], s1.at[d - 1], r1.at[d - 1], self.b, peer))
            self.first[-1].start()

    def to_beams(self):
        s2, r2 = self.sems[2:4]
        own = self.tot[self.block(self.t), :]
        for d, copy in enumerate(self.first):
            copy.wait_recv()
            own = own + self.in_tm[d]
        self.part[...] = own
        self.second = []
        for d in range(1, self.beams):
            peer = lax.rem(self.b + d, self.beams)
            self.second.append(remote(
                self.part, self.in_beam.at[d - 1], s2.at[d - 1], r2.at[d - 1], peer, self.t))
            self.second[-1].start()

    def back(self):
        s3, r3 = self.sems[4:]
        own = self.part[...]
        for d, copy in enumerate(self.second):
            copy.wait_recv()
            own = own + self.in_beam[d]
        self.whole[...] = own
        self.third = []
        for d in range(1, self.tms):
            peer = lax.rem(self.t + d, self.tms)
            self.third.append(remote(
                self.whole, self.res.at[self.block(self.t)], s3.at[d - 1], r3.at[d - 1], self.b, peer))
            self.third[-1].start()
        self.res[self.block(self.t), :] = own

    def arrive(self):
        for copy in self.third:
            copy.wait_recv()

    def leave(self):
        for copy in self.first + self.second + self.third:
            copy.wait_send()


def total_scratch(beams, tms, rows):
    share = (rows // tms, LANES)
    sem = pltpu.SemaphoreType.DMA
    return [
        pltpu.VMEM(share, jnp.float32),
        pltpu.VMEM(share, jnp.float32),
        pltpu.VMEM((tms - 1, *share), jnp.float32),
        pltpu.VMEM((beams - 1, *share), jnp.float32),
        sem((tms - 1,)), sem((tms - 1,)), sem((beams - 1,)), sem((beams - 1,)), sem((tms - 1,)), sem((tms - 1,)),
    ]


TOTAL_SCRATCH = 10


def tables(channels):
    tiles = channels // LANES
    angle = 2.0 * math.pi * (np.outer(np.arange(tiles), np.arange(LANES)) % channels) / channels
    scale = channels ** -0.5
    k2 = np.concatenate([np.arange(0, LANES, 2), np.arange(1, LANES, 2)])
    last = 2.0 * math.pi * (np.outer(np.arange(LANES), k2) % LANES) / LANES
    c, s = np.cos(last), np.sin(last)
    matrix = jnp.asarray(np.block([[c, -s], [s, c]]).astype(np.float32))
    high = matrix.astype(jnp.bfloat16)
    low = (matrix - high.astype(jnp.float32)).astype(jnp.bfloat16)
    return (
        jnp.asarray((scale * np.cos(angle)).astype(np.float32)),
        jnp.asarray((-scale * np.sin(angle)).astype(np.float32)),
        high,
        low,
    )


def times(x, turn, of):
    turn = turn % of
    re, im = x
    if turn == 0:
        return x
    if 4 * turn == of:
        return im, -re
    if 2 * turn == of:
        return -re, -im
    if 4 * turn == 3 * of:
        return -im, re
    c, s = math.cos(2 * math.pi * turn / of), math.sin(2 * math.pi * turn / of)
    if 8 * turn % of == 0:
        h = abs(c)
        if 8 * turn == of:
            return (re + im) * h, (im - re) * h
        if 8 * turn == 3 * of:
            return (im - re) * h, (re + im) * -h
    return re * c + im * s, im * c - re * s


def add(x, y):
    return x[0] + y[0], x[1] + y[1]


def sub(x, y):
    return x[0] - y[0], x[1] - y[1]


def transform(xs):
    n = len(xs)
    if n == 1:
        return xs
    even, odd = transform(xs[0::2]), transform(xs[1::2])
    odd = [times(o, k, n) for k, o in enumerate(odd)]
    return [add(e, o) for e, o in zip(even, odd)] + [sub(e, o) for e, o in zip(even, odd)]


def channelize(lo, hi, taps, tw_re, tw_im, high, low, xs, mid, rows_h, rows_l, pw, turned):
    tap_count, channels = taps.shape
    tiles = channels // LANES
    outer = 8
    inner = tiles // outer

    def first(b, carry):
        tiles_out = []
        for a in range(outer):
            cols = pl.ds(pl.multiple_of((a * inner + b) * LANES, LANES), LANES)
            weights = taps[:, cols]
            pair = []
            for q in range(2):
                base = (a * 2 + q) * 2 * GROUP
                xs[base : base + GROUP, :] = lo[q, :, cols]
                xs[base + GROUP : base + 2 * GROUP, :] = hi[q, :, cols]
                total = weights[0:1] * lo[q, :, cols]
                for t in range(1, tap_count):
                    total = total + weights[t : t + 1] * xs[base + t : base + t + GROUP, :]
                pair.append(total)
            tiles_out.append(tuple(pair))
        for c, z in enumerate(transform(tiles_out)):
            at = pl.ds(pl.multiple_of((c * inner + b) * GROUP, GROUP), GROUP)
            mid[0, at, :] = z[0]
            mid[1, at, :] = z[1]
        return carry

    lax.fori_loop(0, inner, first, 0)

    for c0 in range(0, outer, 2):
        both = []
        for c in (c0, c0 + 1):
            zs = []
            for b in range(inner):
                at = slice((c * inner + b) * GROUP, (c * inner + b + 1) * GROUP)
                zs.append(times((mid[0, at, :], mid[1, at, :]), b * c, tiles))
            turned_out = []
            for d, (re, im) in enumerate(transform(zs)):
                k1 = c + outer * d
                wr, wi = tw_re[k1 : k1 + 1, :], tw_im[k1 : k1 + 1, :]
                turned_out.append((re * wr - im * wi, re * wi + im * wr))
            both.append(turned_out)
        for d in range(inner):
            at = slice((c0 + outer * d) * GROUP, (c0 + outer * d + 2) * GROUP)
            for q in range(2):
                x = jnp.concatenate([both[0][d][q], both[1][d][q]], axis=0)
                h = x.astype(jnp.bfloat16)
                rows_h[at, q * LANES : (q + 1) * LANES] = h
                rows_l[at, q * LANES : (q + 1) * LANES] = (x - h.astype(jnp.float32)).astype(jnp.bfloat16)

    def dot(x, y):
        return jnp.dot(x, y, preferred_element_type=jnp.float32)

    spec = dot(rows_h[...], high[...]) + dot(rows_l[...], high[...]) + dot(rows_h[...], low[...])
    spec_re, spec_im = spec[:, :LANES], spec[:, LANES:]
    pw[...] = spec_re * spec_re + spec_im * spec_im

    left = lax.broadcasted_iota(jnp.int32, (tiles, LANES), 1) < tiles
    total = jnp.zeros((tiles, LANES), jnp.float32)
    for f in range(0, GROUP, 2):
        pair = jnp.concatenate(
            [pw[pl.ds(f, tiles, stride=GROUP), :], pw[pl.ds(f + 1, tiles, stride=GROUP), :]], axis=0
        ).T
        upper, lower = pair[:tiles], pair[tiles:]
        one = jnp.where(left, upper, pltpu.roll(lower, tiles, 1))
        two = jnp.where(left, pltpu.roll(upper, tiles, 1), lower)
        total = total + one + two
        turned[pl.ds(f, tiles, stride=GROUP), :] = one
        turned[pl.ds(f + 1, tiles, stride=GROUP), :] = two
    return total


def kernel(beams, tms, scale, x, *refs):
    from_consts, (powers, base) = refs[:5], refs[5:7]
    refs = refs[7:]
    consts, refs = refs[:5], refs[5:]
    xv, rim, pv, tot, res, load_sem, const_sem, rim_send, rim_recv, out_sem = refs[:10]
    work, refs = refs[10:16], refs[16:]
    pols, _, frames, channels = xv.shape
    groups = frames // GROUP
    tiles = channels // LANES
    turned = work[-1]
    reach = consts[0].shape[0] - 1
    b, t = lax.axis_index("beam"), lax.axis_index("tm")

    loads = [pltpu.make_async_copy(x.at[p], xv.at[p], load_sem.at[p]) for p in range(pols)]
    fetches = [pltpu.make_async_copy(f, c, const_sem.at[i]) for i, (f, c) in enumerate(zip(from_consts, consts))]
    fetches[0].start()
    for copy in loads + fetches[1:]:
        copy.start()
    greet(beams, tms)
    rims = [
        remote(x.at[p, :, 0:reach, :], rim.at[p, :, 0:reach, :], rim_send.at[p], rim_recv.at[p], b, lax.rem(t + tms - 1, tms))
        for p in range(pols)
    ]

    @pl.when(t > 0)
    def _():
        for copy in rims:
            copy.start()

    @pl.when(t == tms - 1)
    def _():
        rim[...] = jnp.zeros_like(rim)

    for copy in fetches + loads:
        copy.wait()

    def one(p, g, lo, hi):
        part = channelize(lo, hi, *consts, *work)
        at = pl.ds(pl.multiple_of(p * tiles, tiles), tiles)
        if isinstance(p, int):
            tot[at, :] = tot[at, :] + part
        else:
            tot[at, :] = jnp.where(g == 0, part, tot[at, :] + part) if groups > 2 else part
        frames_at = pl.ds(pl.multiple_of(g * GROUP, GROUP), GROUP)
        for j in range(tiles):
            pv[p, frames_at, j * LANES : (j + 1) * LANES] = turned[j * GROUP : (j + 1) * GROUP, :]

    def early(i, carry):
        p, g = i // (groups - 1), lax.rem(i, groups - 1)
        after = pl.multiple_of((g + 1) * GROUP, GROUP)
        one(
            p, g,
            xv.at[p, :, pl.ds(pl.multiple_of(g * GROUP, GROUP), GROUP), :],
            xv.at[p, :, pl.ds(after, GROUP), :],
        )
        return carry

    lax.fori_loop(0, pols * (groups - 1), early, 0)

    outs = []
    totals = []
    for p in range(pols):

        @pl.when(t < tms - 1)
        def _():
            rims[p].wait_recv()

        one(p, groups - 1, xv.at[p, :, frames - GROUP : frames, :], rim.at[p])
        now = refs[p * TOTAL_SCRATCH : (p + 1) * TOTAL_SCRATCH]
        totals.append(Total(beams, tms, tot, res, p * tiles, tiles, *now[:4], now[4:]))
        totals[p].to_tm()
        outs.append(pltpu.make_async_copy(pv.at[p], powers.at[p], out_sem.at[p]))
        outs[p].start()
        if p > 0:
            totals[p - 1].back()
        totals[p].to_beams()
    for p in range(pols):
        if p == pols - 1:
            totals[p].back()
        totals[p].arrive()
        for j in range(tiles):
            row = p * tiles + j
            base[p : p + 1, j * LANES : (j + 1) * LANES] = res[row : row + 1, :] * scale
    for total in totals:
        total.leave()

    @pl.when(t > 0)
    def _():
        for copy in rims:
            copy.wait_send()

    for copy in outs:
        copy.wait()


def powers_and_base(x, taps, scale):
    beams, tms = lax.axis_size("beam"), lax.axis_size("tm")
    pols, _, frames, channels = x.shape
    tiles = channels // LANES
    rows = tiles * GROUP
    consts = (taps, *tables(channels))
    sem = pltpu.SemaphoreType.DMA
    f32 = jnp.float32
    anywhere = pl.BlockSpec(memory_space=pl.ANY)
    return pl.pallas_call(
        functools.partial(kernel, beams, tms, scale),
        out_shape=(
            jax.ShapeDtypeStruct((pols, frames, channels), f32),
            jax.ShapeDtypeStruct((pols, channels), f32),
        ),
        in_specs=[pl.BlockSpec(memory_space=pltpu.HBM)] * (1 + len(consts)),
        out_specs=(anywhere, pl.BlockSpec(memory_space=pltpu.VMEM)),
        scratch_shapes=[pltpu.VMEM(c.shape, c.dtype) for c in consts]
        + [
            pltpu.VMEM(x.shape, f32),
            pltpu.VMEM((pols, 2, GROUP, channels), f32),
            pltpu.VMEM((pols, frames, channels), f32),
            pltpu.VMEM((pols * tiles, LANES), f32),
            pltpu.VMEM((pols * tiles, LANES), f32),
            sem((pols,)), sem((len(consts),)), sem((pols,)), sem((pols,)), sem((pols,)),
            pltpu.VMEM((8 * 2 * 2 * GROUP, LANES), f32),
            pltpu.VMEM((2, rows, LANES), f32),
            pltpu.VMEM((rows, 2 * LANES), jnp.bfloat16),
            pltpu.VMEM((rows, 2 * LANES), jnp.bfloat16),
            pltpu.VMEM((rows, LANES), f32),
            pltpu.VMEM((rows, LANES), f32),
        ]
        + total_scratch(beams, tms, tiles) * pols,
        compiler_params=pltpu.CompilerParams(
            collective_id=0, has_side_effects=True
        ),
        name="powers_and_base",
    )(x, *consts)


def body(voltages, filter_taps):
    frames = voltages.shape[3] * lax.axis_size("tm")
    beams = voltages.shape[0] * lax.axis_size("beam")
    powers, base = powers_and_base(voltages[0], filter_taps, 1.0 / (frames * beams))
    return (powers - base[:, None, :])[None]


def solution(mesh):
    placed = (P("beam", None, None, "tm", None), P())
    return jax.shard_map(
        body, mesh=mesh, in_specs=placed, out_specs=P("beam", None, "tm", None), check_vma=False
    )
```

```python
import functools
import math

import jax
import jax.numpy as jnp
import numpy as np
from jax import lax
from jax.experimental import pallas as pl
from jax.experimental.pallas import tpu as pltpu
from jax.sharding import PartitionSpec as P

LANES = 128
GROUP = 8


def remote(src, dst, send, recv, beam, tm):
    return pltpu.make_async_remote_copy(
        src_ref=src, dst_ref=dst, send_sem=send, recv_sem=recv,
        device_id=(beam, tm), device_id_type=pl.DeviceIdType.MESH,
    )


def greet(beams, tms):
    b, t = lax.axis_index("beam"), lax.axis_index("tm")
    barrier = pltpu.get_barrier_semaphore()
    for d in range(1, tms):
        pl.semaphore_signal(barrier, inc=1, device_id=(b, lax.rem(t + d, tms)), device_id_type=pl.DeviceIdType.MESH)
    for d in range(1, beams):
        pl.semaphore_signal(barrier, inc=1, device_id=(lax.rem(b + d, beams), t), device_id_type=pl.DeviceIdType.MESH)
    pl.semaphore_wait(barrier, tms - 1 + beams - 1)


class Total:
    def __init__(self, beams, tms, tot, res, first_row, count, part, whole, in_tm, in_beam, sems):
        self.beams, self.tms, self.tot, self.res = beams, tms, tot, res
        self.first_row, self.rows = first_row, count // tms
        self.part, self.whole, self.in_tm, self.in_beam, self.sems = part, whole, in_tm, in_beam, sems
        self.b, self.t = lax.axis_index("beam"), lax.axis_index("tm")
        self.sent = []

    def block(self, i):
        return pl.ds(pl.multiple_of(self.first_row + i * self.rows, self.rows), self.rows)

    def to_tm(self):
        s1, r1 = self.sems[:2]
        self.first = []
        for d in range(1, self.tms):
            peer = lax.rem(self.t + d, self.tms)
            self.first.append(remote(
                self.tot.at[self.block(peer)], self.in_tm.at[d - 1], s1.at[d - 1], r1.at[d - 1], self.b, peer))
            self.first[-1].start()

    def to_beams(self):
        s2, r2 = self.sems[2:4]
        own = self.tot[self.block(self.t), :]
        for d, copy in enumerate(self.first):
            copy.wait_recv()
            own = own + self.in_tm[d]
        self.part[...] = own
        self.second = []
        for d in range(1, self.beams):
            peer = lax.rem(self.b + d, self.beams)
            self.second.append(remote(
                self.part, self.in_beam.at[d - 1], s2.at[d - 1], r2.at[d - 1], peer, self.t))
            self.second[-1].start()

    def back(self):
        s3, r3 = self.sems[4:]
        own = self.part[...]
        for d, copy in enumerate(self.second):
            copy.wait_recv()
            own = own + self.in_beam[d]
        self.whole[...] = own
        self.third = []
        for d in range(1, self.tms):
            peer = lax.rem(self.t + d, self.tms)
            self.third.append(remote(
                self.whole, self.res.at[self.block(self.t)], s3.at[d - 1], r3.at[d - 1], self.b, peer))
            self.third[-1].start()
        self.res[self.block(self.t), :] = own

    def arrive(self):
        for copy in self.third:
            copy.wait_recv()

    def leave(self):
        for copy in self.first + self.second + self.third:
            copy.wait_send()


def total_scratch(beams, tms, rows):
    share = (rows // tms, LANES)
    sem = pltpu.SemaphoreType.DMA
    return [
        pltpu.VMEM(share, jnp.float32),
        pltpu.VMEM(share, jnp.float32),
        pltpu.VMEM((tms - 1, *share), jnp.float32),
        pltpu.VMEM((beams - 1, *share), jnp.float32),
        sem((tms - 1,)), sem((tms - 1,)), sem((beams - 1,)), sem((beams - 1,)), sem((tms - 1,)), sem((tms - 1,)),
    ]


TOTAL_SCRATCH = 10


def tables(channels):
    tiles = channels // LANES
    angle = 2.0 * math.pi * (np.outer(np.arange(tiles), np.arange(LANES)) % channels) / channels
    scale = channels ** -0.5
    k2 = np.concatenate([np.arange(0, LANES, 2), np.arange(1, LANES, 2)])
    last = 2.0 * math.pi * (np.outer(np.arange(LANES), k2) % LANES) / LANES
    c, s = np.cos(last), np.sin(last)
    matrix = jnp.asarray(np.block([[c, -s], [s, c]]).astype(np.float32))
    high = matrix.astype(jnp.bfloat16)
    low = (matrix - high.astype(jnp.float32)).astype(jnp.bfloat16)
    return (
        jnp.asarray((scale * np.cos(angle)).astype(np.float32)),
        jnp.asarray((-scale * np.sin(angle)).astype(np.float32)),
        high,
        low,
    )


def times(x, turn, of):
    turn = turn % of
    re, im = x
    if turn == 0:
        return x
    if 4 * turn == of:
        return im, -re
    if 2 * turn == of:
        return -re, -im
    if 4 * turn == 3 * of:
        return -im, re
    c, s = math.cos(2 * math.pi * turn / of), math.sin(2 * math.pi * turn / of)
    if 8 * turn % of == 0:
        h = abs(c)
        if 8 * turn == of:
            return (re + im) * h, (im - re) * h
        if 8 * turn == 3 * of:
            return (im - re) * h, (re + im) * -h
    return re * c + im * s, im * c - re * s


def add(x, y):
    return x[0] + y[0], x[1] + y[1]


def sub(x, y):
    return x[0] - y[0], x[1] - y[1]


def transform(xs):
    n = len(xs)
    if n == 1:
        return xs
    even, odd = transform(xs[0::2]), transform(xs[1::2])
    odd = [times(o, k, n) for k, o in enumerate(odd)]
    return [add(e, o) for e, o in zip(even, odd)] + [sub(e, o) for e, o in zip(even, odd)]


def channelize(lo, hi, taps, tw_re, tw_im, high, low, xs, mid, rows_h, rows_l, pw, turned):
    tap_count, channels = taps.shape
    tiles = channels // LANES
    outer = 8
    inner = tiles // outer

    def first(b, carry):
        tiles_out = []
        for a in range(outer):
            cols = pl.ds(pl.multiple_of((a * inner + b) * LANES, LANES), LANES)
            weights = taps[:, cols]
            pair = []
            for q in range(2):
                base = (a * 2 + q) * 2 * GROUP
                xs[base : base + GROUP, :] = lo[q, :, cols]
                xs[base + GROUP : base + 2 * GROUP, :] = hi[q, :, cols]
                total = weights[0:1] * lo[q, :, cols]
                for t in range(1, tap_count):
                    total = total + weights[t : t + 1] * xs[base + t : base + t + GROUP, :]
                pair.append(total)
            tiles_out.append(tuple(pair))
        for c, z in enumerate(transform(tiles_out)):
            at = pl.ds(pl.multiple_of((c * inner + b) * GROUP, GROUP), GROUP)
            mid[0, at, :] = z[0]
            mid[1, at, :] = z[1]
        return carry

    lax.fori_loop(0, inner, first, 0)

    for c0 in range(0, outer, 2):
        both = []
        for c in (c0, c0 + 1):
            zs = []
            for b in range(inner):
                at = slice((c * inner + b) * GROUP, (c * inner + b + 1) * GROUP)
                zs.append(times((mid[0, at, :], mid[1, at, :]), b * c, tiles))
            turned_out = []
            for d, (re, im) in enumerate(transform(zs)):
                k1 = c + outer * d
                wr, wi = tw_re[k1 : k1 + 1, :], tw_im[k1 : k1 + 1, :]
                turned_out.append((re * wr - im * wi, re * wi + im * wr))
            both.append(turned_out)
        for d in range(inner):
            at = slice((c0 + outer * d) * GROUP, (c0 + outer * d + 2) * GROUP)
            for q in range(2):
                x = jnp.concatenate([both[0][d][q], both[1][d][q]], axis=0)
                h = x.astype(jnp.bfloat16)
                rows_h[at, q * LANES : (q + 1) * LANES] = h
                rows_l[at, q * LANES : (q + 1) * LANES] = (x - h.astype(jnp.float32)).astype(jnp.bfloat16)

    def dot(x, y):
        return jnp.dot(x, y, preferred_element_type=jnp.float32)

    spec = dot(rows_h[...], high[...]) + dot(rows_l[...], high[...]) + dot(rows_h[...], low[...])
    spec_re, spec_im = spec[:, :LANES], spec[:, LANES:]
    pw[...] = spec_re * spec_re + spec_im * spec_im

    left = lax.broadcasted_iota(jnp.int32, (tiles, LANES), 1) < tiles
    total = jnp.zeros((tiles, LANES), jnp.float32)
    for f in range(0, GROUP, 2):
        pair = jnp.concatenate(
            [pw[pl.ds(f, tiles, stride=GROUP), :], pw[pl.ds(f + 1, tiles, stride=GROUP), :]], axis=0
        ).T
        upper, lower = pair[:tiles], pair[tiles:]
        one = jnp.where(left, upper, pltpu.roll(lower, tiles, 1))
        two = jnp.where(left, pltpu.roll(upper, tiles, 1), lower)
        total = total + one + two
        turned[pl.ds(f, tiles, stride=GROUP), :] = one
        turned[pl.ds(f + 1, tiles, stride=GROUP), :] = two
    return total


def kernel(beams, tms, scale, x, *refs):
    from_consts, (powers, base) = refs[:5], refs[5:7]
    refs = refs[7:]
    consts, refs = refs[:5], refs[5:]
    xv, rim, pv, tot, res, load_sem, const_sem, rim_send, rim_recv, out_sem = refs[:10]
    work, refs = refs[10:16], refs[16:]
    pols, _, frames, channels = xv.shape
    groups = frames // GROUP
    tiles = channels // LANES
    turned = work[-1]
    reach = consts[0].shape[0] - 1
    b, t = lax.axis_index("beam"), lax.axis_index("tm")

    loads = [pltpu.make_async_copy(x.at[p], xv.at[p], load_sem.at[p]) for p in range(pols)]
    fetches = [pltpu.make_async_copy(f, c, const_sem.at[i]) for i, (f, c) in enumerate(zip(from_consts, consts))]
    for copy in loads + fetches:
        copy.start()
    greet(beams, tms)
    rims = [
        remote(xv.at[p, :, 0:reach, :], rim.at[p, :, 0:reach, :], rim_send.at[p], rim_recv.at[p], b, lax.rem(t + tms - 1, tms))
        for p in range(pols)
    ]

    for load, copy in zip(loads, rims):
        load.wait()
        pl.when(t > 0)(copy.start)

    @pl.when(t == tms - 1)
    def _():
        rim[...] = jnp.zeros_like(rim)

    for copy in fetches:
        copy.wait()

    def one(p, g, lo, hi):
        part = channelize(lo, hi, *consts, *work)
        at = pl.ds(pl.multiple_of(p * tiles, tiles), tiles)
        if isinstance(p, int):
            tot[at, :] = tot[at, :] + part
        else:
            tot[at, :] = jnp.where(g == 0, part, tot[at, :] + part) if groups > 2 else part
        frames_at = pl.ds(pl.multiple_of(g * GROUP, GROUP), GROUP)
        for j in range(tiles):
            pv[p, frames_at, j * LANES : (j + 1) * LANES] = turned[j * GROUP : (j + 1) * GROUP, :]

    def early(i, carry):
        p, g = i // (groups - 1), lax.rem(i, groups - 1)
        after = pl.multiple_of((g + 1) * GROUP, GROUP)
        one(
            p, g,
            xv.at[p, :, pl.ds(pl.multiple_of(g * GROUP, GROUP), GROUP), :],
            xv.at[p, :, pl.ds(after, GROUP), :],
        )
        return carry

    lax.fori_loop(0, pols * (groups - 1), early, 0)

    outs = []
    totals = []
    for p in range(pols):

        @pl.when(t < tms - 1)
        def _():
            rims[p].wait_recv()

        one(p, groups - 1, xv.at[p, :, frames - GROUP : frames, :], rim.at[p])
        now = refs[p * TOTAL_SCRATCH : (p + 1) * TOTAL_SCRATCH]
        totals.append(Total(beams, tms, tot, res, p * tiles, tiles, *now[:4], now[4:]))
        totals[p].to_tm()
        outs.append(pltpu.make_async_copy(pv.at[p], powers.at[p], out_sem.at[p]))
        outs[p].start()
        if p > 0:
            totals[p - 1].back()
        totals[p].to_beams()
    for p in range(pols):
        if p == pols - 1:
            totals[p].back()
        totals[p].arrive()
        for j in range(tiles):
            row = p * tiles + j
            base[p : p + 1, j * LANES : (j + 1) * LANES] = res[row : row + 1, :] * scale
    for total in totals:
        total.leave()

    @pl.when(t > 0)
    def _():
        for copy in rims:
            copy.wait_send()

    for copy in outs:
        copy.wait()


def powers_and_base(x, taps, scale):
    beams, tms = lax.axis_size("beam"), lax.axis_size("tm")
    pols, _, frames, channels = x.shape
    tiles = channels // LANES
    rows = tiles * GROUP
    consts = (taps, *tables(channels))
    sem = pltpu.SemaphoreType.DMA
    f32 = jnp.float32
    anywhere = pl.BlockSpec(memory_space=pl.ANY)
    return pl.pallas_call(
        functools.partial(kernel, beams, tms, scale),
        out_shape=(
            jax.ShapeDtypeStruct((pols, frames, channels), f32),
            jax.ShapeDtypeStruct((pols, channels), f32),
        ),
        in_specs=[pl.BlockSpec(memory_space=pltpu.HBM)] * (1 + len(consts)),
        out_specs=(anywhere, pl.BlockSpec(memory_space=pltpu.VMEM)),
        scratch_shapes=[pltpu.VMEM(c.shape, c.dtype) for c in consts]
        + [
            pltpu.VMEM(x.shape, f32),
            pltpu.VMEM((pols, 2, GROUP, channels), f32),
            pltpu.VMEM((pols, frames, channels), f32),
            pltpu.VMEM((pols * tiles, LANES), f32),
            pltpu.VMEM((pols * tiles, LANES), f32),
            sem((pols,)), sem((len(consts),)), sem((pols,)), sem((pols,)), sem((pols,)),
            pltpu.VMEM((8 * 2 * 2 * GROUP, LANES), f32),
            pltpu.VMEM((2, rows, LANES), f32),
            pltpu.VMEM((rows, 2 * LANES), jnp.bfloat16),
            pltpu.VMEM((rows, 2 * LANES), jnp.bfloat16),
            pltpu.VMEM((rows, LANES), f32),
            pltpu.VMEM((rows, LANES), f32),
        ]
        + total_scratch(beams, tms, tiles) * pols,
        compiler_params=pltpu.CompilerParams(
            collective_id=0, has_side_effects=True
        ),
        name="powers_and_base",
    )(x, *consts)


def body(voltages, filter_taps):
    frames = voltages.shape[3] * lax.axis_size("tm")
    beams = voltages.shape[0] * lax.axis_size("beam")
    powers, base = powers_and_base(voltages[0], filter_taps, 1.0 / (frames * beams))
    return (powers - base[:, None, :])[None]


def solution(mesh):
    placed = (P("beam", None, None, "tm", None), P())
    return jax.shard_map(
        body, mesh=mesh, in_specs=placed, out_specs=P("beam", None, "tm", None), check_vma=False
    )
```
